32 devices in a mesh: gx: 4 (over x, core), gy: 2 (over y), gz: 4 (over z).
Axes of the slice: x: 2, y: 2, z: 4, core: 2. Of those that a mesh axis runs over, the one named last changes fastest.
Arguments:
- fields: float32 [32, 32, 16, 512], P(None, 'gx', 'gy', 'gz'), may hold values from -8 to 8
- strength: float32 [32], replicated, may hold values from 0.3 to 1
Outputs:
- filtered: float32 [32, 32, 16, 512], P(None, 'gx', 'gy', 'gz')
The draws below stay inside these ranges and needn't reach their ends.
All inputs are finite; a program needn't handle non-finite values.
Results may differ from the reference program's by a relative error of at most 0.00002.
Values sent between devices are 32-bit elements; how exact they have to be, the bound alone decides.
No kernel may reach another device: no remote copies, remote signals or barrier semaphores. Data moves between devices by JAX's collectives and lax.ppermute only.
A program may use at most 64 MiB of HBM per device.

```python
import math
import jax
import jax.numpy as jnp
from jax import lax

SPECIES = 32
NX = 32
NY = 16
NZ = 512


def steps_of(own_key, extent, shards, smallest, top_value):
    def one(axis_at, shards_of):
        draws = jax.random.uniform(jax.random.fold_in(jax.random.fold_in(own_key, 6), axis_at), (shards_of,), jnp.float32, smallest / len(shards), top_value / len(shards))
        return jnp.repeat(jnp.exp(draws), extent[axis_at] // shards_of).reshape((-1,) + (1,) * (len(extent) - axis_at - 1))

    gain = one(*shards[0])
    for cut in shards[1:]:
        gain = gain * one(*cut)
    return gain


def scatter_about(own_key, shape, scale, reach, split=(), kind=jnp.bfloat16):
    values = jax.random.normal(own_key, shape, jnp.float32) * scale
    if len(split) > 0:
        values = steps_of(own_key, shape, split, -0.22, 0.18) * values
    return jnp.clip(values, min=-reach, max=reach).astype(kind)


def setup_inputs(seed: int = 0) -> dict:
    key_of = jax.random.split(jax.random.key(seed), 3)
    fields = scatter_about(key_of[0], (SPECIES, NX, NY, NZ), 1.0, 8.0, ((1, 4), (2, 2), (3, 4)), jnp.float32)
    strength = jnp.clip(jnp.exp(jax.random.uniform(key_of[1], (SPECIES,), jnp.float32, math.log(0.3), math.log(1.0))), 0.3, 1.0)
    return {"fields": fields, "strength": strength}


filter_weights = [1.0, -10.0, 45.0, -120.0, 210.0, -252.0, 210.0, -120.0, 45.0, -10.0, 1.0]


def tenth_difference(field, axis):
    total = jnp.zeros(field.shape, jnp.float32)
    for index in range(11):
        total = total + filter_weights[index] * jnp.roll(field, 5 - index, axis)
    return total


def filter_species(packed):
    field, scale = packed
    summed = tenth_difference(field, 0) + tenth_difference(field, 1) + tenth_difference(field, 2)
    return field + (scale / 1024.0) * summed


def reference(fields, strength):
    return lax.map(filter_species, (fields, strength))
```

```python
import functools

import jax
import jax.numpy as jnp
import numpy as np
from jax import lax
from jax.experimental import pallas as pl
from jax.experimental.pallas import tpu as pltpu
from jax.sharding import PartitionSpec as P

WEIGHTS = (1.0, -10.0, 45.0, -120.0, 210.0, -252.0, 210.0, -120.0, 45.0, -10.0, 1.0)
HALF = 5
EDGE = 8
ANY = pl.BlockSpec(memory_space=pl.ANY)
SMEM = pl.BlockSpec(memory_space=pltpu.SMEM)


def band(rows, cols, offset):
    m = np.zeros((rows, cols), np.float32)
    for i in range(rows):
        for j in range(cols):
            d = offset + j - i
            if -HALF <= d <= HALF:
                m[i, j] = WEIGHTS[HALF + d]
    return m


def diagonals(matrix):
    n = matrix.shape[0]
    found = []
    for m in range(n):
        coef = np.array([matrix[i, (i + m) % n] for i in range(n)], np.float32)
        if np.any(coef):
            found.append((m, coef))
    return found


def column(values, cells, lanes):
    row = lax.broadcasted_iota(jnp.int32, (cells, lanes), 0)
    out = jnp.full((cells, lanes), float(values[0]), jnp.float32)
    for i in range(1, cells):
        if values[i] != values[i - 1]:
            out = jnp.where(row >= i, float(values[i]), out)
    return out


def along_y(block, diags):
    cells, lanes = block.shape[-2:]
    total = None
    for m, coef in diags:
        moved = block if m == 0 else pltpu.roll(block, (cells - m) % cells, block.ndim - 2)
        term = moved * column(coef, cells, lanes)
        total = term if total is None else total + term
    return total


def thirds(x):
    a = x.astype(jnp.bfloat16)
    rest = x - a.astype(jnp.float32)
    b = rest.astype(jnp.bfloat16)
    c = (rest - b.astype(jnp.float32)).astype(jnp.bfloat16)
    return a, b, c


def dot(a, b, dims):
    return lax.dot_general(a, b, (dims, ((), ())), preferred_element_type=jnp.float32)


def edges_kernel(pick_ref, u_ref, head_ref, tail_ref, low_ref, high_ref):
    block = u_ref[...]
    n, cx, cy, cz = block.shape
    head_ref[...] = block[:, :HALF]
    tail_ref[...] = block[:, cx - HALF:]
    rows = block.reshape(n * cx * cy, cz)
    edge = None
    for part in thirds(rows):
        term = dot(pick_ref[...], part, ((1,), (1,)))
        edge = term if edge is None else edge + term
    low_ref[...] = edge[:EDGE]
    high_ref[...] = edge[EDGE:]


def inner_kernel(own_y, scale_ref, band_ref, rim_ref, u_ref, before_ref, after_ref, low_ref, high_ref, out_ref):
    n, cx, cy, cz = u_ref.shape
    first = pl.program_id(0) * n
    rows = u_ref[...].reshape(n * cx * cy, cz)
    total = None
    for part in thirds(rows):
        term = dot(part, band_ref[...], ((1,), (0,)))
        total = term if total is None else total + term
    rim = jnp.concatenate([low_ref[...], high_ref[...]], axis=0)
    for part in thirds(rim):
        total = total + dot(part, rim_ref[...], ((0,), (0,)))
    total = total.reshape(n, cx, cy, cz)
    for s in range(n):
        planes = [before_ref[s, i] for i in range(HALF)] + [u_ref[s, i] for i in range(cx)]
        planes = planes + [after_ref[s, i] for i in range(HALF)]
        scale = scale_ref[first + s]
        for i in range(cx):
            here = planes[i + HALF]
            acc = WEIGHTS[HALF] * here
            for k in range(1, HALF + 1):
                acc = acc + WEIGHTS[HALF + k] * (planes[i + HALF - k] + planes[i + HALF + k])
            acc = acc + along_y(here, own_y) + total[s, i]
            out_ref[s, i] = here + scale * acc


def outer_kernel(sides, scale_ref, *refs):
    partial_ref, out_ref = refs[-2], refs[-1]
    n, cx = out_ref.shape[:2]
    first = pl.program_id(0) * n
    for s in range(n):
        scale = scale_ref[first + s]
        for i in range(cx):
            acc = None
            for ref, diags in zip(refs[:-2], sides):
                term = along_y(ref[s, i], diags)
                acc = term if acc is None else acc + term
            out_ref[s, i] = partial_ref[s, i] + scale * acc


def ring(axis, step):
    count = lax.axis_size(axis)
    return [(i, (i + step) % count) for i in range(count)]


def local(fields, strength):
    ns, cx, cy, cz = fields.shape
    block = 4
    grid = (ns // block,)
    rows = block * cx * cy
    f32 = jnp.float32

    def cells(width):
        return pl.BlockSpec((block, width, cy, cz), lambda b: (b, 0, 0, 0))

    whole = cells(cx)
    edge_spec = pl.BlockSpec((EDGE, rows), lambda b: (0, b))

    def fixed(a):
        return pl.BlockSpec(a.shape, lambda b: (0,) * a.ndim)

    def cost(flops, size):
        return pl.CostEstimate(flops=flops, bytes_accessed=size, transcendentals=0)

    if lax.axis_size("gy") == 2:
        other = lax.ppermute(fields, "gy", ring("gy", 1))
        y_in = [other]
        sides = [diagonals(band(cy, cy, -cy) + band(cy, cy, cy))]
    else:
        up = lax.ppermute(fields[:, :, cy - HALF:], "gy", ring("gy", 1))
        down = lax.ppermute(fields[:, :, :HALF], "gy", ring("gy", -1))
        gap = cy - HALF
        y_in = [jnp.pad(up, ((0, 0), (0, 0), (gap, 0), (0, 0))), jnp.pad(down, ((0, 0), (0, 0), (0, gap), (0, 0)))]
        sides = [diagonals(band(cy, cy, -cy)), diagonals(band(cy, cy, cy))]

    pick = np.zeros((2 * EDGE, cz), np.float32)
    rim = np.zeros((2 * EDGE, cz), np.float32)
    for i in range(HALF):
        pick[i, i] = 1.0
        pick[EDGE + i, cz - HALF + i] = 1.0
        for j in range(cz):
            for row, d in ((i, i - HALF - j), (EDGE + i, cz + i - j)):
                if -HALF <= d <= HALF:
                    rim[row, j] = WEIGHTS[HALF + d]
    pick = jnp.asarray(pick, jnp.bfloat16)
    rim = jnp.asarray(rim, jnp.bfloat16)
    band_z = jnp.asarray(band(cz, cz, 0), jnp.bfloat16)

    size = fields.size * 4
    head, tail, low, high = pl.pallas_call(
        edges_kernel,
        grid=grid,
        in_specs=[fixed(pick), whole],
        out_specs=[cells(HALF), cells(HALF), edge_spec, edge_spec],
        out_shape=[
            jax.ShapeDtypeStruct((ns, HALF, cy, cz), f32),
            jax.ShapeDtypeStruct((ns, HALF, cy, cz), f32),
            jax.ShapeDtypeStruct((EDGE, ns * cx * cy), f32),
            jax.ShapeDtypeStruct((EDGE, ns * cx * cy), f32),
        ],
        cost_estimate=cost(size, 2 * size),
        name="edges",
    )(pick, fields)
    before = lax.ppermute(tail, "gx", ring("gx", 1))
    after = lax.ppermute(head, "gx", ring("gx", -1))
    from_low = lax.ppermute(high, "gz", ring("gz", 1))
    from_high = lax.ppermute(low, "gz", ring("gz", -1))

    scale = strength / 1024.0
    partial = pl.pallas_call(
        functools.partial(inner_kernel, diagonals(band(cy, cy, 0))),
        grid=grid,
        in_specs=[SMEM, fixed(band_z), fixed(rim), whole, cells(HALF), cells(HALF), edge_spec, edge_spec],
        out_specs=whole,
        out_shape=jax.ShapeDtypeStruct(fields.shape, f32),
        cost_estimate=cost(20 * size, 3 * size),
        name="inner",
    )(scale, band_z, rim, fields, before, after, from_low, from_high)
    return pl.pallas_call(
        functools.partial(outer_kernel, sides),
        grid=grid,
        in_specs=[SMEM] + [whole] * (len(y_in) + 1),
        out_specs=whole,
        out_shape=jax.ShapeDtypeStruct(fields.shape, f32),
        cost_estimate=cost(5 * size, 3 * size),
        name="outer",
    )(scale, *y_in, partial)


def solution(mesh):
    return jax.shard_map(
        local,
        mesh=mesh,
        in_specs=(P(None, "gx", "gy", "gz"), P()),
        out_specs=P(None, "gx", "gy", "gz"),
        check_vma=False,
    )
```

```python
import functools

import jax
import jax.numpy as jnp
import numpy as np
from jax import lax
from jax.experimental import pallas as pl
from jax.experimental.pallas import tpu as pltpu
from jax.sharding import PartitionSpec as P

WEIGHTS = (1.0, -10.0, 45.0, -120.0, 210.0, -252.0, 210.0, -120.0, 45.0, -10.0, 1.0)
HALF = 5
EDGE = 8
ANY = pl.BlockSpec(memory_space=pl.ANY)
SMEM = pl.BlockSpec(memory_space=pltpu.SMEM)
VMEM = pl.BlockSpec(memory_space=pltpu.VMEM)
HBM = pl.BlockSpec(memory_space=pltpu.HBM)
GRANT = 16 * 1024 * 1024


def band(rows, cols, offset):
    m = np.zeros((rows, cols), np.float32)
    for i in range(rows):
        for j in range(cols):
            d = offset + j - i
            if -HALF <= d <= HALF:
                m[i, j] = WEIGHTS[HALF + d]
    return m


def diagonals(matrix):
    n = matrix.shape[0]
    found = []
    for m in range(n):
        coef = np.array([matrix[i, (i + m) % n] for i in range(n)], np.float32)
        if np.any(coef):
            found.append((m, coef))
    return found


def column(values, cells, lanes):
    row = lax.broadcasted_iota(jnp.int32, (cells, lanes), 0)
    out = jnp.full((cells, lanes), float(values[0]), jnp.float32)
    for i in range(1, cells):
        if values[i] != values[i - 1]:
            out = jnp.where(row >= i, float(values[i]), out)
    return out


def along_y(block, diags):
    cells, lanes = block.shape[-2:]
    total = None
    for m, coef in diags:
        moved = block if m == 0 else pltpu.roll(block, (cells - m) % cells, block.ndim - 2)
        term = moved * (coef if coef.ndim == 2 else column(coef, cells, lanes))
        total = term if total is None else total + term
    return total


def thirds(x):
    a = x.astype(jnp.bfloat16)
    rest = x - a.astype(jnp.float32)
    b = rest.astype(jnp.bfloat16)
    c = (rest - b.astype(jnp.float32)).astype(jnp.bfloat16)
    return a, b, c


def dot(a, b, dims):
    return lax.dot_general(a, b, (dims, ((), ())), preferred_element_type=jnp.float32)


def slices_kernel(u_ref, head_ref, tail_ref, sems):
    cx = u_ref.shape[1]
    copies = [
        pltpu.make_async_copy(u_ref.at[:, pl.ds(cx - HALF, HALF)], tail_ref, sems.at[0]),
        pltpu.make_async_copy(u_ref.at[:, pl.ds(0, HALF)], head_ref, sems.at[1]),
    ]
    for copy in copies:
        copy.start()
    for copy in copies:
        copy.wait()


def edges_kernel(u_ref, low_ref, high_ref):
    ns, cx, cy, cz = u_ref.shape
    step = cz // (cx * cy)

    def body(b, carry):
        rows = u_ref[pl.ds(b * step, step)].reshape(cz, cz)
        turned = rows.T
        at = pl.ds(pl.multiple_of(b * cz, cz), cz)
        low_ref[:, at] = turned[:EDGE]
        high_ref[:, at] = turned[cz - EDGE:]
        return carry

    lax.fori_loop(0, ns // step, body, 0, unroll=2)


def inner_kernel(own_y, block, scale_ref, band_ref, rim_ref, u_ref, low_ref, high_ref, out_ref):
    ns, cx, cy, cz = u_ref.shape
    count = block * cx * cy

    def body(b, carry):
        u = u_ref[pl.ds(b * block, block)]
        rows = u.reshape(count, cz)
        at = pl.ds(pl.multiple_of(b * count, count), count)
        rim = jnp.concatenate(thirds(jnp.concatenate([low_ref[:, at], high_ref[:, at]], axis=0)), axis=0)
        total = dot(rim, rim_ref[...], ((0,), (0,)))
        total = total + dot(jnp.concatenate(thirds(rows), axis=1), band_ref[...], ((1,), (0,)))
        total = total.reshape(block, cx, cy, cz)
        for s in range(block):
            scale = scale_ref[b * block + s]
            for i in range(cx):
                here = u[s, i]
                out_ref[b * block + s, i] = here + scale * (along_y(here, own_y) + total[s, i])
        return carry

    lax.fori_loop(0, ns // block, body, 0)


def cross_kernel(scale_ref, u_ref, before_ref, after_ref, partial_ref, out_ref):
    ns, cx = u_ref.shape[:2]

    def body(s, carry):
        planes = [before_ref[s, i] for i in range(HALF)] + [u_ref[s, i] for i in range(cx)]
        planes = planes + [after_ref[s, i] for i in range(HALF)]
        scale = scale_ref[s]
        for i in range(cx):
            acc = WEIGHTS[HALF] * planes[i + HALF]
            for k in range(1, HALF + 1):
                acc = acc + WEIGHTS[HALF + k] * (planes[i + HALF - k] + planes[i + HALF + k])
            out_ref[s, i] = partial_ref[s, i] + scale * acc
        return carry

    lax.fori_loop(0, ns, body, 0)


def outer_kernel(sides, groups, scale_ref, *refs):
    partial_ref, out_ref, done_ref, sems = refs[-4:]
    ns, cx, cy, cz = partial_ref.shape
    size = ns // groups
    sides = [[(m, column(coef, cy, cz)) for m, coef in diags] for diags in sides]
    copies = []
    for g in range(groups):
        at = pl.ds(g * size, size)

        def body(s, carry):
            scale = scale_ref[s]
            for i in range(cx):
                acc = None
                for ref, diags in zip(refs[:-4], sides):
                    term = along_y(ref[s, i], diags)
                    acc = term if acc is None else acc + term
                done_ref[s, i] = partial_ref[s, i] + scale * acc
            return carry

        lax.fori_loop(g * size, (g + 1) * size, body, 0)
        copy = pltpu.make_async_copy(done_ref.at[at], out_ref.at[at], sems.at[g])
        copy.start()
        copies.append(copy)
    for copy in copies:
        copy.wait()


def ring(axis, step):
    count = lax.axis_size(axis)
    return [(i, (i + step) % count) for i in range(count)]


def local(fields, strength):
    ns, cx, cy, cz = fields.shape
    f32 = jnp.float32
    size = fields.size * 4

    def call(kernel, name, flops, out, n_in, scratch=(), scalars=1, in_space=VMEM, out_space=VMEM, **more):
        return pl.pallas_call(
            kernel,
            in_specs=[SMEM] * scalars + [in_space] * n_in,
            out_specs=[out_space] * len(out),
            out_shape=[jax.ShapeDtypeStruct(shape, f32) for shape in out],
            scratch_shapes=list(scratch),
            cost_estimate=pl.CostEstimate(flops=flops, bytes_accessed=size, transcendentals=0),
            compiler_params=pltpu.CompilerParams(vmem_limit_bytes=GRANT),
            name=name,
            **more,
        )

    if lax.axis_size("gy") == 2:
        y_in = [lax.ppermute(fields, "gy", ring("gy", 1))]
        sides = [diagonals(band(cy, cy, -cy) + band(cy, cy, cy))]
    else:
        up = lax.ppermute(fields[:, :, cy - HALF:], "gy", ring("gy", 1))
        down = lax.ppermute(fields[:, :, :HALF], "gy", ring("gy", -1))
        gap = cy - HALF
        y_in = [jnp.pad(up, ((0, 0), (0, 0), (gap, 0), (0, 0))), jnp.pad(down, ((0, 0), (0, 0), (0, gap), (0, 0)))]
        sides = [diagonals(band(cy, cy, -cy)), diagonals(band(cy, cy, cy))]

    layers = (ns, HALF, cy, cz)
    head, tail = call(
        slices_kernel, "slices", size, [layers] * 2, 1, [pltpu.SemaphoreType.DMA((2,))], scalars=0, in_space=HBM
    )(fields)
    before = lax.ppermute(tail, "gx", ring("gx", 1))
    after = lax.ppermute(head, "gx", ring("gx", -1))

    edge = (EDGE, ns * cx * cy)
    low, high = call(edges_kernel, "edges", size, [edge] * 2, 1, scalars=0)(fields)
    from_low = lax.ppermute(high, "gz", ring("gz", 1))
    from_high = lax.ppermute(low, "gz", ring("gz", -1))

    rim = np.zeros((2 * EDGE, cz), np.float32)
    for i in range(EDGE):
        for j in range(cz):
            for row, d in ((i, i - EDGE - j), (EDGE + i, cz + i - j)):
                if -HALF <= d <= HALF:
                    rim[row, j] = WEIGHTS[HALF + d]
    rim = jnp.asarray(np.tile(rim, (3, 1)), jnp.bfloat16)
    band_z = jnp.asarray(np.tile(band(cz, cz, 0), (3, 1)), jnp.bfloat16)

    scale = strength / 1024.0
    inner = functools.partial(inner_kernel, diagonals(band(cy, cy, 0)), 4)
    (partial,) = call(inner, "inner", 20 * size, [fields.shape], 5)(scale, band_z, rim, fields, from_low, from_high)
    (partial,) = call(cross_kernel, "cross", 5 * size, [fields.shape], 4, input_output_aliases={4: 0})(
        scale, fields, before, after, partial
    )
    groups = 4
    outer = functools.partial(outer_kernel, sides, groups)
    (out,) = call(
        outer,
        "outer",
        5 * size,
        [fields.shape],
        len(y_in) + 1,
        [pltpu.VMEM(fields.shape, f32), pltpu.SemaphoreType.DMA((groups,))],
        out_space=ANY,
    )(scale, *y_in, partial)
    return out


def solution(mesh):
    return jax.shard_map(
        local,
        mesh=mesh,
        in_specs=(P(None, "gx", "gy", "gz"), P()),
        out_specs=P(None, "gx", "gy", "gz"),
        check_vma=False,
    )
```

```python
import functools

import jax
import jax.numpy as jnp
import numpy as np
from jax import lax
from jax.experimental import pallas as pl
from jax.experimental.pallas import tpu as pltpu
from jax.sharding import PartitionSpec as P

WEIGHTS = (1.0, -10.0, 45.0, -120.0, 210.0, -252.0, 210.0, -120.0, 45.0, -10.0, 1.0)
HALF = 5
EDGE = 8
ANY = pl.BlockSpec(memory_space=pl.ANY)
SMEM = pl.BlockSpec(memory_space=pltpu.SMEM)
VMEM = pl.BlockSpec(memory_space=pltpu.VMEM)
HBM = pl.BlockSpec(memory_space=pltpu.HBM)
GROUPS = (12, 20, 28)
UNROLL = 4
GRANT = 16 * 1024 * 1024


def band(rows, cols, offset):
    m = np.zeros((rows, cols), np.float32)
    for i in range(rows):
        for j in range(cols):
            d = offset + j - i
            if -HALF <= d <= HALF:
                m[i, j] = WEIGHTS[HALF + d]
    return m


def terms(matrix):
    n = matrix.shape[0]
    left = matrix.copy()
    found = []
    for m in range(n):
        at = (np.arange(n), (np.arange(n) + m) % n)
        if np.count_nonzero(left[at]) > n // 2:
            found.append((at[1], left[at].copy()))
            left[at] = 0.0
    while np.any(left):
        source, coef = np.arange(n), np.zeros(n, np.float32)
        for i in range(n):
            if np.any(left[i]):
                source[i] = np.flatnonzero(left[i])[0]
                coef[i] = left[i, source[i]]
                left[i, source[i]] = 0.0
        found.append((source, coef))
    return found


def column(values, cells, lanes, kind):
    row = lax.broadcasted_iota(jnp.int32, (cells, lanes), 0)
    out = jnp.full((cells, lanes), values[0].item(), kind)
    for i in range(1, cells):
        if values[i] != values[i - 1]:
            out = jnp.where(row >= i, values[i].item(), out)
    return out


def prepared(rows, cells, lanes):
    out = []
    for source, coef in rows:
        shift = int(source[0])
        if not np.array_equal(source, (np.arange(cells) + shift) % cells):
            shift = column(source, cells, lanes, jnp.int32)
        out.append((shift, column(coef, cells, lanes, jnp.float32)))
    return out


def along_y(block, rows):
    cells = block.shape[0]
    total = None
    for shift, coef in rows:
        if not isinstance(shift, int):
            moved = jnp.take_along_axis(block, shift, axis=0, mode="promise_in_bounds")
        else:
            moved = pltpu.roll(block, cells - shift, 0) if shift else block
        total = moved * coef if total is None else total + moved * coef
    return total


def thirds(x):
    a = x.astype(jnp.bfloat16)
    rest = x - a.astype(jnp.float32)
    b = rest.astype(jnp.bfloat16)
    c = (rest - b.astype(jnp.float32)).astype(jnp.bfloat16)
    return a, b, c


def dot(a, b, dims):
    return lax.dot_general(a, b, (dims, ((), ())), preferred_element_type=jnp.float32)


def slices_kernel(u_ref, head_ref, tail_ref, sems):
    cx = u_ref.shape[1]
    copies = [
        pltpu.make_async_copy(u_ref.at[:, pl.ds(cx - HALF, HALF)], tail_ref, sems.at[0]),
        pltpu.make_async_copy(u_ref.at[:, pl.ds(0, HALF)], head_ref, sems.at[1]),
    ]
    for copy in copies:
        copy.start()
    for copy in copies:
        copy.wait()


def edges_kernel(u_ref, low_ref, high_ref):
    ns, cx, cy, cz = u_ref.shape
    step = cz // (cx * cy)

    def body(b, carry):
        rows = u_ref[pl.ds(b * step, step)].reshape(cz, cz)
        turned = rows.T
        at = pl.ds(pl.multiple_of(b * cz, cz), cz)
        low_ref[:, at] = turned[:EDGE]
        high_ref[:, at] = turned[cz - EDGE:]
        return carry

    lax.fori_loop(0, ns // step, body, 0, unroll=2)


def inner_kernel(own_y, block, scale_ref, band_ref, rim_ref, u_ref, low_ref, high_ref, out_ref):
    ns, cx, cy, cz = u_ref.shape
    count = block * cx * cy
    own_y = prepared(own_y, cy, cz)

    def body(b, carry):
        u = u_ref[pl.ds(b * block, block)]
        rows = u.reshape(count, cz)
        at = pl.ds(pl.multiple_of(b * count, count), count)
        rim = jnp.concatenate(thirds(jnp.concatenate([low_ref[:, at], high_ref[:, at]], axis=0)), axis=0)
        total = dot(rim, rim_ref[...], ((0,), (0,)))
        total = total + dot(jnp.concatenate(thirds(rows), axis=1), band_ref[...], ((1,), (0,)))
        total = total.reshape(block, cx, cy, cz)
        for s in range(block):
            scale = scale_ref[pl.ds(b * block + s, 1), :]
            for i in range(cx):
                here = u[s, i]
                out_ref[b * block + s, i] = here + scale * (along_y(here, own_y) + total[s, i])
        return carry

    lax.fori_loop(0, ns // block, body, 0)


def cross_kernel(scale_ref, u_ref, before_ref, after_ref, partial_ref, out_ref):
    ns, cx = u_ref.shape[:2]

    def body(s, carry):
        planes = [before_ref[s, i] for i in range(HALF)] + [u_ref[s, i] for i in range(cx)]
        planes = planes + [after_ref[s, i] for i in range(HALF)]
        scale = scale_ref[pl.ds(s, 1), :]
        for i in range(cx):
            acc = WEIGHTS[HALF] * planes[i + HALF]
            for k in range(1, HALF + 1):
                acc = acc + WEIGHTS[HALF + k] * (planes[i + HALF - k] + planes[i + HALF + k])
            out_ref[s, i] = partial_ref[s, i] + scale * acc
        return carry

    lax.fori_loop(0, ns, body, 0)


def outer_kernel(sides, cuts, scale_ref, partial_ref, *refs):
    y_refs = refs[:-3]
    out_ref, done_ref, sems = refs[-3:]
    cx, cy, cz = partial_ref.shape[1:]
    sides = [prepared(rows, cy, cz) for rows in sides]
    copies = []
    for g, (low, high) in enumerate(zip(cuts[:-1], cuts[1:])):

        def body(s, carry):
            scale = scale_ref[pl.ds(s, 1), :]
            for i in range(cx):
                acc = None
                for ref, rows in zip(y_refs, sides):
                    term = along_y(ref[s, i], rows)
                    acc = term if acc is None else acc + term
                done_ref[s, i] = partial_ref[s, i] + scale * acc
            return carry

        lax.fori_loop(low, high, body, 0, unroll=UNROLL)
        at = pl.ds(low, high - low)
        copy = pltpu.make_async_copy(done_ref.at[at], out_ref.at[at], sems.at[g])
        copy.start()
        copies.append(copy)
    for copy in copies:
        copy.wait()


def ring(axis, step):
    count = lax.axis_size(axis)
    return [(i, (i + step) % count) for i in range(count)]


def local(fields, strength):
    ns, cx, cy, cz = fields.shape
    f32 = jnp.float32
    size = fields.size * 4

    def call(kernel, name, flops, out, n_in, scratch=(), in_space=VMEM, out_space=VMEM, **more):
        return pl.pallas_call(
            kernel,
            in_specs=in_space if isinstance(in_space, list) else [in_space] * n_in,
            out_specs=[out_space] * len(out),
            out_shape=[jax.ShapeDtypeStruct(shape, f32) for shape in out],
            scratch_shapes=list(scratch),
            cost_estimate=pl.CostEstimate(flops=flops, bytes_accessed=size, transcendentals=0),
            compiler_params=pltpu.CompilerParams(vmem_limit_bytes=GRANT),
            name=name,
            **more,
        )

    if lax.axis_size("gy") == 2:
        y_in = [lax.ppermute(fields, "gy", ring("gy", 1))]
        sides = [terms(band(cy, cy, -cy) + band(cy, cy, cy))]
    else:
        up = lax.ppermute(fields[:, :, cy - HALF:], "gy", ring("gy", 1))
        down = lax.ppermute(fields[:, :, :HALF], "gy", ring("gy", -1))
        gap = cy - HALF
        y_in = [jnp.pad(up, ((0, 0), (0, 0), (gap, 0), (0, 0))), jnp.pad(down, ((0, 0), (0, 0), (0, gap), (0, 0)))]
        sides = [terms(band(cy, cy, -cy)), terms(band(cy, cy, cy))]

    layers = (ns, HALF, cy, cz)
    head, tail = call(
        slices_kernel, "slices", size, [layers] * 2, 1, [pltpu.SemaphoreType.DMA((2,))], in_space=HBM
    )(fields)
    before = lax.ppermute(tail, "gx", ring("gx", 1))
    after = lax.ppermute(head, "gx", ring("gx", -1))

    edge = (EDGE, ns * cx * cy)
    low, high = call(edges_kernel, "edges", size, [edge] * 2, 1)(fields)
    from_low = lax.ppermute(high, "gz", ring("gz", 1))
    from_high = lax.ppermute(low, "gz", ring("gz", -1))

    rim = np.zeros((2 * EDGE, cz), np.float32)
    for i in range(EDGE):
        for j in range(cz):
            for row, d in ((i, i - EDGE - j), (EDGE + i, cz + i - j)):
                if -HALF <= d <= HALF:
                    rim[row, j] = WEIGHTS[HALF + d]
    rim = jnp.asarray(np.tile(rim, (3, 1)), jnp.bfloat16)
    band_z = jnp.asarray(np.tile(band(cz, cz, 0), (3, 1)), jnp.bfloat16)

    scale = jnp.broadcast_to((strength / 1024.0)[:, None], (ns, cz))
    inner = functools.partial(inner_kernel, terms(band(cy, cy, 0)), 4)
    (partial,) = call(inner, "inner", 20 * size, [fields.shape], 6)(scale, band_z, rim, fields, from_low, from_high)
    (partial,) = call(cross_kernel, "cross", 5 * size, [fields.shape], 5, input_output_aliases={4: 0})(
        scale, fields, before, after, partial
    )
    cuts = [0] + sorted({ns * c // 32 for c in GROUPS} - {0, ns}) + [ns]
    outer = functools.partial(outer_kernel, sides, cuts)
    (out,) = call(
        outer,
        "outer",
        5 * size,
        [fields.shape],
        2 + len(y_in),
        [pltpu.VMEM(fields.shape, f32), pltpu.SemaphoreType.DMA((len(cuts) - 1,))],
        out_space=HBM,
    )(scale, partial, *y_in)
    return out


def solution(mesh):
    return jax.shard_map(
        local,
        mesh=mesh,
        in_specs=(P(None, "gx", "gy", "gz"), P()),
        out_specs=P(None, "gx", "gy", "gz"),
        check_vma=False,
    )
```
